8 devices in a mesh: fsdp: 2 (over z, y), ep: 4 (over x, core).
Axes of the slice: x: 2, y: 2, z: 1, core: 2. Of those that a mesh axis runs over, the one named last changes fastest.
Arguments:
- grad_out: bfloat16 [8192, 1536], P(('fsdp', 'ep'))
- expert_idx: int32 [8192, 8], P(('fsdp', 'ep'))
- slot_pos: int32 [8192, 8], P(('fsdp', 'ep'))
- gates: float32 [8192, 8], P(('fsdp', 'ep'))
- x_disp: bfloat16 [40, 2048, 1536], P('ep', 'fsdp')
- h_gate: bfloat16 [40, 2048, 512], P('ep', 'fsdp')
- h_up: bfloat16 [40, 2048, 512], P('ep', 'fsdp')
- y_disp: bfloat16 [40, 2048, 1536], P('ep', 'fsdp')
- w_gate: bfloat16 [40, 1536, 512], P('ep', 'fsdp')
- w_down: bfloat16 [40, 512, 1536], P('ep', 'fsdp')
- w_up: bfloat16 [40, 1536, 512], P('ep', 'fsdp')
Outputs:
- output 1: bfloat16 [8192, 1536], P(('fsdp', 'ep'))
- output 2: float32 [8192, 8], P(('fsdp', 'ep'))
- output 3: float32 [40, 1536, 512], P('ep', 'fsdp')
- output 4: float32 [40, 512, 1536], P('ep', 'fsdp')
- output 5: float32 [40, 1536, 512], P('ep', 'fsdp')
All inputs are finite; a program needn't handle non-finite values.
Results may differ from the reference program's by a relative error of at most 0.00111.
Values are sent between devices in bfloat16 or wider.
A program may use at most 1 GiB of HBM per device.

```python
import jax
import jax.numpy as jnp
from jax import lax

D = 1536
F = 512
EXPERTS = 40
TOP = 8
TOK = 1024
NDEV = 8
CAP = 256


def route_draw(key):
    key_bias, key_noise, key_hot = jax.random.split(key, 3)
    expert_ids = jnp.arange(EXPERTS, dtype=jnp.int32)
    expert_bias = jax.random.randint(key_bias, (EXPERTS,), 0, 512, dtype=jnp.int32)
    noise_int = jax.random.randint(key_noise, (NDEV, TOK, EXPERTS), 0, 1024, dtype=jnp.int32)
    hot_expert = jax.random.randint(key_hot, (NDEV,), 0, EXPERTS, dtype=jnp.int32)
    forced = (jnp.arange(TOK, dtype=jnp.int32)[None, :, None] <= CAP) & (expert_ids[None, None, :] == hot_expert[:, None, None])
    score_int = (noise_int + expert_bias + jnp.where(forced, 4096, 0)) * EXPERTS + expert_ids
    expert_idx = lax.top_k(score_int, TOP)[1].astype(jnp.int32)

    def block_slots(block_idx):
        flat_ids = block_idx.reshape(-1)
        hit_mask = (flat_ids[:, None] == expert_ids[None, :]).astype(jnp.int32)
        slot_rank = jnp.sum((jnp.cumsum(hit_mask, axis=0) - hit_mask) * hit_mask, axis=1)
        return jnp.where(slot_rank < CAP, slot_rank, -1).reshape(TOK, TOP)

    slot_pos = lax.map(block_slots, expert_idx)
    return expert_idx.reshape(NDEV * TOK, TOP), slot_pos.reshape(NDEV * TOK, TOP).astype(jnp.int32)


def setup_inputs(seed: int = 0) -> dict:
    keys = jax.random.split(jax.random.key(seed), 11)
    expert_idx, slot_pos = route_draw(keys[0])
    rows_all = NDEV * CAP
    grad_out = jax.random.normal(keys[1], (NDEV * TOK, D), jnp.float32).astype(jnp.bfloat16)
    gates = jax.random.uniform(keys[2], (NDEV * TOK, TOP), jnp.float32, 0.2, 1.0)
    x_disp = jax.random.normal(keys[3], (EXPERTS, rows_all, D), jnp.float32).astype(jnp.bfloat16)
    h_gate = jax.random.normal(keys[4], (EXPERTS, rows_all, F), jnp.float32).astype(jnp.bfloat16)
    h_up = jax.random.normal(keys[5], (EXPERTS, rows_all, F), jnp.float32).astype(jnp.bfloat16)
    y_disp = (0.25 * jax.random.normal(keys[6], (EXPERTS, rows_all, D), jnp.float32)).astype(jnp.bfloat16)
    w_gate = (jax.random.normal(keys[7], (EXPERTS, D, F), jnp.float32) * D ** -0.5).astype(jnp.bfloat16)
    w_down = (jax.random.normal(keys[8], (EXPERTS, F, D), jnp.float32) * F ** -0.5).astype(jnp.bfloat16)
    w_up = (jax.random.normal(keys[9], (EXPERTS, D, F), jnp.float32) * D ** -0.5).astype(jnp.bfloat16)
    return {'grad_out': grad_out, 'expert_idx': expert_idx, 'slot_pos': slot_pos, 'gates': gates, 'x_disp': x_disp, 'h_gate': h_gate, 'h_up': h_up, 'y_disp': y_disp, 'w_gate': w_gate, 'w_down': w_down, 'w_up': w_up}


def expert_backward(operands):
    dy_rows, gate_rows, x_rows, pre_gate, pre_up, y_rows, w_gate, w_down, w_up = operands
    g_rows = (dy_rows.astype(jnp.float32) * gate_rows[:, None]).astype(jnp.bfloat16)
    gate_pre = pre_gate.astype(jnp.float32)
    up_pre = pre_up.astype(jnp.float32)
    sigmoid_gate = jax.nn.sigmoid(gate_pre)
    silu_gate = gate_pre * sigmoid_gate
    act_rows = (silu_gate * up_pre).astype(jnp.bfloat16)
    d_act = jnp.dot(g_rows, w_down.T, preferred_element_type=jnp.float32)
    dh_gate = (d_act * up_pre * sigmoid_gate * (1.0 + gate_pre * (1.0 - sigmoid_gate))).astype(jnp.bfloat16)
    dh_up = (d_act * silu_gate).astype(jnp.bfloat16)
    dx_rows = (jnp.dot(dh_gate, w_gate.T, preferred_element_type=jnp.float32) + jnp.dot(dh_up, w_up.T, preferred_element_type=jnp.float32)).astype(jnp.bfloat16)
    dgate_rows = jnp.sum(dy_rows.astype(jnp.float32) * y_rows.astype(jnp.float32), axis=1)
    dw_gate = jnp.dot(x_rows.T, dh_gate, preferred_element_type=jnp.float32)
    dw_down = jnp.dot(act_rows.T, g_rows, preferred_element_type=jnp.float32)
    dw_up = jnp.dot(x_rows.T, dh_up, preferred_element_type=jnp.float32)
    return dx_rows, dgate_rows, dw_gate, dw_down, dw_up


def reference(grad_out, expert_idx, slot_pos, gates, x_disp, h_gate, h_up, y_disp, w_gate, w_down, w_up):
    rows_all = NDEV * CAP
    choices = NDEV * TOK * TOP
    block_ids = jnp.arange(NDEV * TOK, dtype=jnp.int32)[:, None] // TOK
    dest_row = jnp.where(slot_pos >= 0, expert_idx * rows_all + block_ids * CAP + slot_pos, EXPERTS * rows_all).reshape(-1)
    src_choice = jnp.full((EXPERTS * rows_all,), choices, jnp.int32).at[dest_row].set(jnp.arange(choices, dtype=jnp.int32), mode='drop')
    dy_rows = jnp.take(grad_out, src_choice // TOP, axis=0, mode='fill', fill_value=0).reshape(EXPERTS, rows_all, D)
    gate_rows = jnp.take(gates.reshape(-1), src_choice, mode='fill', fill_value=0).reshape(EXPERTS, rows_all)
    dx_rows, dgate_rows, dw_gate, dw_down, dw_up = lax.map(expert_backward, (dy_rows, gate_rows, x_disp, h_gate, h_up, y_disp, w_gate, w_down, w_up))
    picked = jnp.take(dx_rows.reshape(EXPERTS * rows_all, D), dest_row, axis=0, mode='fill', fill_value=0).reshape(NDEV * TOK, TOP, D)
    grad_x = jnp.sum(picked.astype(jnp.float32), axis=1).astype(jnp.bfloat16)
    grad_gates = jnp.take(dgate_rows.reshape(-1), dest_row, mode='fill', fill_value=0).reshape(NDEV * TOK, TOP)
    return grad_x, grad_gates, dw_gate, dw_down, dw_up
```

```python
import functools

import jax
import jax.numpy as jnp
from jax import lax
from jax.experimental import pallas as pl
from jax.experimental.pallas import tpu as pltpu
from jax.sharding import PartitionSpec as P


F32 = jnp.float32
BF16 = jnp.bfloat16


def dot(a, b, dims):
    return lax.dot_general(a, b, (dims, ((), ())), preferred_element_type=F32)


def rows_kernel(has_y, has_init, *refs):
    q_ref, dy_ref, meta_ref = refs[:3]
    refs = refs[3:]
    if has_y:
        y_ref, refs = refs[0], refs[1:]
    if has_init:
        init_ref, refs = refs[0], refs[1:]
    hg_ref, hu_ref, w2_ref, w1_ref, w3_ref, dx_ref, dh1_ref, dh3_ref, dw2_ref = refs[:9]
    refs = refs[9:]
    if has_y:
        gg_ref, refs = refs[0], refs[1:]
    (acc_ref,) = refs
    n, e = pl.program_id(0), pl.program_id(1)
    cap, tok = hg_ref.shape[1], dy_ref.shape[1]
    half = acc_ref.shape[1]

    slot = meta_ref[0, 0, 0:1, :].astype(jnp.int32)
    gate = meta_ref[0, 0, 1:2, :]
    hit = lax.broadcasted_iota(jnp.int32, (cap, tok), 0) == slot
    pick = jnp.where(hit, 1.0, 0.0).astype(BF16)
    s = jnp.sum(jnp.where(hit, gate, 0.0), axis=1, keepdims=True)
    dy = dot(pick, dy_ref[0], ((1,), (0,)))
    if has_y:
        gg = jnp.sum(dy * y_ref[0].astype(F32), axis=1, keepdims=True)
        gg_ref[0, 0] = jnp.sum(jnp.where(hit, gg, 0.0), axis=0, keepdims=True)
    g = (dy * s).astype(BF16)
    h1 = hg_ref[0].astype(F32)
    h3 = hu_ref[0].astype(F32)
    sig = jax.nn.sigmoid(h1)
    silu = h1 * sig
    da = dot(g, w2_ref[0], ((1,), (1,)))
    dh1 = (da * h3 * sig * (1.0 + h1 * (1.0 - sig))).astype(BF16)
    dh3 = (da * silu).astype(BF16)
    dh1_ref[0] = dh1
    dh3_ref[0] = dh3
    a = jnp.where(s > 0.0, silu * h3, 0.0)
    a = jnp.where(q_ref[0] == 0, a[:, :half], a[:, half:]).astype(BF16)
    dw2 = dot(a, g, ((0,), (0,)))
    dx = dot(dh1, w1_ref[0], ((1,), (1,))) + dot(dh3, w3_ref[0], ((1,), (1,)))
    back = dot(pick, dx.astype(BF16), ((0,), (0,)))

    @pl.when(e == 0)
    def _():
        dx_ref[0] = back

    @pl.when(e != 0)
    def _():
        dx_ref[0] += back

    @pl.when(n == 0)
    def _():
        acc_ref[e] = dw2

    @pl.when(n != 0)
    def _():
        acc_ref[e] += dw2

    @pl.when(n == pl.num_programs(0) - 1)
    def _():
        if has_init:
            dw2_ref[0] = acc_ref[e] + init_ref[0]
        else:
            dw2_ref[0] = acc_ref[e]


def rows_back(q, dy, meta, y, init, hg, hu, w2, w1, w3):
    blocks, tok, width = dy.shape
    e_loc, rows, ff = hg.shape
    cap = rows // blocks
    wh = w1.shape[1]
    fh = ff // 2
    has_y, has_init = y is not None, init is not None
    last = blocks - 1
    row = lambda n, e, q_ref: (e, n, 0)
    per_e = lambda n, e, q_ref: (e, 0, 0)
    late_e = lambda n, e, q_ref: (jnp.where(n == last, e, 0), 0, 0)
    in_specs = [pl.BlockSpec((1, tok, width), lambda n, e, q_ref: (n, 0, 0)), pl.BlockSpec((1, 1, 2, tok), lambda n, e, q_ref: (n, e, 0, 0))]
    args = [dy, meta]
    if has_y:
        in_specs.append(pl.BlockSpec((1, cap, width), row))
        args.append(y)
    if has_init:
        in_specs.append(pl.BlockSpec((1, fh, width), late_e))
        args.append(init)
    in_specs += [pl.BlockSpec((1, cap, ff), row), pl.BlockSpec((1, cap, ff), row), pl.BlockSpec((1, ff, width), per_e), pl.BlockSpec((1, wh, ff), per_e), pl.BlockSpec((1, wh, ff), per_e)]
    args += [hg, hu, w2, w1, w3]
    out_shape = [jax.ShapeDtypeStruct((blocks, tok, wh), F32), jax.ShapeDtypeStruct((e_loc, rows, ff), BF16), jax.ShapeDtypeStruct((e_loc, rows, ff), BF16), jax.ShapeDtypeStruct((e_loc, fh, width), F32)]
    out_specs = [pl.BlockSpec((1, tok, wh), lambda n, e, q_ref: (n, 0, 0)), pl.BlockSpec((1, cap, ff), row), pl.BlockSpec((1, cap, ff), row), pl.BlockSpec((1, fh, width), late_e)]
    if has_y:
        out_shape.append(jax.ShapeDtypeStruct((blocks, e_loc, 1, tok), F32))
        out_specs.append(pl.BlockSpec((1, 1, 1, tok), lambda n, e, q_ref: (n, e, 0, 0)))
    steps = blocks * e_loc
    flops = 2 * steps * cap * (tok * width + width * ff + fh * width + 2 * wh * ff + tok * wh)
    return pl.pallas_call(
        functools.partial(rows_kernel, has_y, has_init),
        out_shape=out_shape,
        grid_spec=pltpu.PrefetchScalarGridSpec(num_scalar_prefetch=1, grid=(blocks, e_loc), in_specs=in_specs, out_specs=out_specs, scratch_shapes=[pltpu.VMEM((e_loc, fh, width), F32)]),
        compiler_params=pltpu.CompilerParams(dimension_semantics=("arbitrary", "arbitrary"), vmem_limit_bytes=62 * 1024 * 1024),
        cost_estimate=pl.CostEstimate(flops=flops, bytes_accessed=200_000_000, transcendentals=0),
        name="rows_back",
    )(q, *args)


def weights_kernel(q_ref, xo_ref, xp_ref, d1o_ref, d1p_ref, d3o_ref, d3p_ref, *refs):
    w1_ref, w3_ref = refs[-2:]
    xo, xp = xo_ref[0], xp_ref[0]
    over = ((0,), (0,))
    w1_ref[0] = dot(xo, d1o_ref[0], over) + dot(xp, d1p_ref[0], over)
    w3_ref[0] = dot(xo, d3o_ref[0], over) + dot(xp, d3p_ref[0], over)


def weights_back(q, first, x, xp, d1o, d1p, d3o, d3p, prev):
    e_loc, rows, _ = x.shape
    count, _, wh = xp.shape
    ff = d1o.shape[2]
    here = lambda e, q_ref: (e + first, 0, 0)
    in_specs = [pl.BlockSpec((1, rows, wh), lambda e, q_ref: (e + first, 0, q_ref[0])), pl.BlockSpec((1, rows, wh), lambda e, q_ref: (e, 0, 0))] + [pl.BlockSpec((1, rows, ff), here)] * 4
    args = [x, xp, d1o, d1p, d3o, d3p]
    aliases = {}
    if prev is not None:
        in_specs += [pl.BlockSpec(memory_space=pl.ANY)] * 2
        args += list(prev)
        aliases = {7: 0, 8: 1}
    return pl.pallas_call(
        weights_kernel,
        out_shape=[jax.ShapeDtypeStruct((e_loc, wh, ff), F32)] * 2,
        grid_spec=pltpu.PrefetchScalarGridSpec(num_scalar_prefetch=1, grid=(count,), in_specs=in_specs, out_specs=[pl.BlockSpec((1, wh, ff), here)] * 2),
        input_output_aliases=aliases,
        compiler_params=pltpu.CompilerParams(dimension_semantics=("arbitrary",), vmem_limit_bytes=62 * 1024 * 1024),
        cost_estimate=pl.CostEstimate(flops=8 * count * rows * wh * ff, bytes_accessed=count * 12_000_000, transcendentals=0),
        name="weights_back",
    )(q, *args)


def solution(mesh):
    ep_n = mesh.shape['ep']
    tok_spec = P(('fsdp', 'ep'), None)
    row_spec = P('ep', 'fsdp', None)
    swap = [(0, 1), (1, 0)]

    def local_backward(grad_out, expert_idx, slot_pos, gates, x_disp, h_gate, h_up, y_disp, w_gate, w_down, w_up):
        tok_n, _ = expert_idx.shape
        e_loc, rows_loc, width = x_disp.shape
        e_all = e_loc * ep_n
        wh = width // 2
        q_idx = lax.axis_index('fsdp')
        q = q_idx.astype(jnp.int32).reshape(1)

        ids = jnp.arange(e_all, dtype=jnp.int32)[:, None, None]
        idx_t, slot_t, gates_t = expert_idx.T, slot_pos.T, gates.T
        hit = (idx_t[None] == ids) & (slot_t[None] >= 0)
        slot_map = jnp.max(jnp.where(hit, slot_t[None], -1), axis=1).astype(F32)
        gate_map = jnp.sum(jnp.where(hit, gates_t[None], 0.0), axis=1)
        meta = jnp.stack([slot_map, gate_map], axis=1).reshape(ep_n, e_loc, 2, tok_n)

        def across(a):
            return lax.ppermute(a, 'fsdp', swap)

        meta_own = lax.all_to_all(meta, 'ep', 0, 0, tiled=True)
        meta_par = lax.all_to_all(across(meta), 'ep', 0, 0, tiled=True)

        def ep_sum(a):
            p = lax.axis_index('ep')
            for bit in (1, 2):
                far = (p // bit) % 2
                a = a.reshape((-1, 2) + a.shape[1:]) if bit == 1 else a.reshape((2, -1) + a.shape[1:])
                axis = 1 if bit == 1 else 0
                send = lax.dynamic_index_in_dim(a, 1 - far, axis, keepdims=False)
                keep = lax.dynamic_index_in_dim(a, far, axis, keepdims=False)
                got = lax.ppermute(send, 'ep', [(i, i ^ bit) for i in range(ep_n)])
                a = keep + got
            return a.reshape(a.shape[-2:])

        w2_par = across(w_down)
        dy_par1 = across(grad_out)
        hg_par = across(h_gate)
        hu_par = across(h_up)
        cuts = [(0, 4), (4, 8), (8, e_loc)]
        x_par = []
        for lo, hi in cuts:
            part = lax.dynamic_slice(x_disp, (lo, 0, (1 - q_idx) * wh), (hi - lo, rows_loc, wh))
            x_par.append(across(part))

        dy_own = lax.all_gather(grad_out, 'ep', axis=0)
        dy_par = lax.all_gather(dy_par1, 'ep', axis=0)
        w2 = jnp.where(q_idx == 0, jnp.concatenate([w_down, w2_par], axis=1), jnp.concatenate([w2_par, w_down], axis=1))

        dx_own, d1o, d3o, dw2_own, gg = rows_back(q, dy_own, meta_own, y_disp, None, h_gate, h_up, w2, w_gate, w_up)
        dx_own = ep_sum(dx_own)
        gg = lax.all_to_all(gg.reshape(ep_n, e_loc, tok_n), 'ep', 0, 0, tiled=True).reshape(e_all, tok_n)
        dx_par, d1p, d3p, grad_w_down = rows_back(q, dy_par, meta_par, None, dw2_own, hg_par, hu_par, w2, w_gate, w_up)
        dx_par = ep_sum(dx_par)
        mine = dx_own.astype(BF16)
        other = across(dx_par.astype(BF16))
        grad_x = jnp.where(q_idx == 0, jnp.concatenate([mine, other], axis=1), jnp.concatenate([other, mine], axis=1))
        grad_gates = jnp.sum(jnp.where(hit, gg[:, None, :], 0.0), axis=0).T

        prev = None
        for (lo, hi), xp in zip(cuts, x_par):
            prev = weights_back(q, lo, x_disp, xp, d1o, d1p, d3o, d3p, prev)
        grad_w_gate, grad_w_up = prev
        return grad_x, grad_gates, grad_w_gate, grad_w_down, grad_w_up

    return jax.shard_map(local_backward, mesh=mesh, in_specs=(tok_spec, tok_spec, tok_spec, tok_spec, row_spec, row_spec, row_spec, row_spec, row_spec, row_spec, row_spec), out_specs=(tok_spec, tok_spec, row_spec, row_spec, row_spec), check_vma=False)
```
